32 devices in a mesh: row: 8 (over z, y), col: 4 (over x, core).
Axes of the slice: x: 2, y: 2, z: 4, core: 2. Of those that a mesh axis runs over, the one named last changes fastest.
Arguments:
- params: float32 [4, 4096, 10240], P(None, ('row', 'col'))
- grads: bfloat16 [4, 4096, 10240], P(None, ('row', 'col')), may hold values from -6 to 6
- row_state_old: float32 [4, 4096], P(None, ('row', 'col')), may hold values from 0.05 to 0.5
- col_state_old: float32 [4, 10240], P(None, ('row', 'col')), may hold values from 0.05 to 0.5
- old_map: int32 [4, 32], replicated, may hold values from 0 to 31, each once within a row
- new_map: int32 [4, 32], replicated, may hold values from 0 to 31, each once within a row
Outputs:
- new_params: float32 [4, 4096, 10240], P(None, 'row', 'col')
- step_change: float32 [4, 4096, 10240], P(None, 'row', 'col')
- row_state: float32 [4, 4096], P(None, ('row', 'col'))
- col_state: float32 [4, 10240], P(None, ('row', 'col'))
The draws below stay inside these ranges and needn't reach their ends.
Inputs may be any that keep to these rules, and one draw needn't show every extreme that they name: Each row of old_map is a permutation of 0 to 31. Each row of new_map is a permutation of 0 to 31.
All inputs are finite; a program needn't handle non-finite values.
Results may differ from the reference program's by a relative error of at most 0.0003.
Values may be sent and summed in bfloat16 or wider, within the bound.
No kernel may reach another device: no remote copies, remote signals or barrier semaphores. Data moves between devices by JAX's collectives and lax.ppermute only.
A program may use at most 192 MiB of HBM per device.

```python
import math
import jax
import jax.numpy as jnp
from jax import lax

D = 4096
FF = 10240
STEP = 4
NMAT = 4
BLOCKS = 32


def draw_params(key, part):
    first_key = jax.random.fold_in(jax.random.fold_in(key, 11), 0)
    rising = 0.5 * 3.0 ** (jnp.arange(D, dtype=jnp.float32) / D)
    values = jax.random.normal(first_key, (NMAT, D, FF), jnp.float32)
    return (values * rising[None, :, None]).astype(jnp.float32)


def steps_of(key, shape, cuts, least, top_value):
    gain, own = 1.0, jax.random.fold_in(key, 6)
    for dim, parts in cuts:
        steps = jnp.exp(jax.random.uniform(jax.random.fold_in(own, dim), (parts,), jnp.float32, least / len(cuts), top_value / len(cuts)))
        gain = gain * jnp.repeat(steps, shape[dim] // parts).reshape([-1 if axis == dim else 1 for axis in range(len(shape))])
    return gain


def scatter_about(stream_key, shape, deviation, limit, shards=(), kind=jnp.bfloat16):
    drawn = deviation * jax.random.normal(stream_key, shape, jnp.float32)
    if shards:
        drawn = drawn * steps_of(stream_key, shape, shards, -0.22, 0.18)
    return jnp.clip(drawn, -limit, limit).astype(kind)


def setup_inputs(seed: int = 0) -> dict:
    arg_keys = jax.random.split(jax.random.key(seed), 7)
    return {
        "params": draw_params(jax.random.fold_in(arg_keys[6], 71), 0),
        "grads": scatter_about(arg_keys[1], (NMAT, D, FF), 1.0, 6.0, ((1, 32),)),
        "row_state_old": jnp.clip(jnp.exp(math.log(0.5) - 2.3025851 * jax.random.uniform(arg_keys[2], (NMAT, D), jnp.float32) ** steps_of(arg_keys[2], (NMAT, D), ((1, 32),), -0.2, 0.2)), 0.05, 0.5),
        "col_state_old": jnp.clip(jnp.exp(math.log(0.5) - 2.3025851 * jax.random.uniform(arg_keys[3], (NMAT, FF), jnp.float32) ** steps_of(arg_keys[3], (NMAT, FF), ((1, 32),), -0.2, 0.2)), 0.05, 0.5),
        "old_map": jax.vmap(lambda own: jax.random.permutation(own, BLOCKS))(jax.random.split(arg_keys[4], NMAT)).reshape((NMAT, BLOCKS)).astype(jnp.int32),
        "new_map": jax.vmap(lambda own: jax.random.permutation(own, BLOCKS))(jax.random.split(arg_keys[5], NMAT)).reshape((NMAT, BLOCKS)).astype(jnp.int32),
    }


eps_square = 1e-30
clip_limit = 1.0

def unpermute(stored, order):
    matrices = stored.shape[0]
    pieces = stored.reshape(matrices, order.shape[1], -1)
    inverse = jnp.argsort(order, axis=1).astype(jnp.int32)
    return jnp.take_along_axis(pieces, inverse[:, :, None], axis=1).reshape(matrices, -1)

def permute(logical, order):
    matrices = logical.shape[0]
    pieces = logical.reshape(matrices, order.shape[1], -1)
    return jnp.take_along_axis(pieces, order[:, :, None], axis=1).reshape(matrices, -1)

def reference(params, grads, row_state_old, col_state_old, old_map, new_map):
    decay_rate = 1.0 - float(STEP) ** (-0.8)
    step_rate = min(0.01, 1.0 / math.sqrt(STEP))
    row_old = unpermute(row_state_old, old_map)
    col_old = unpermute(col_state_old, old_map)
    gradient = grads.astype(jnp.float32)
    squares = gradient * gradient + eps_square
    row_new = decay_rate * row_old + (1.0 - decay_rate) * lax.optimization_barrier(jnp.sum(squares, axis=2)) / FF
    col_new = decay_rate * col_old + (1.0 - decay_rate) * lax.optimization_barrier(jnp.sum(squares, axis=1)) / D
    row_mean = lax.optimization_barrier(jnp.mean(row_new, axis=1))
    variance = row_new[:, :, None] * col_new[:, None, :] / row_mean[:, None, None]
    update = gradient / jnp.sqrt(variance)
    clip_factor = jnp.maximum(1.0, jnp.sqrt(jnp.mean(update * update)) / clip_limit)
    param_scale = jnp.sqrt(lax.optimization_barrier(jnp.mean(params * params, axis=(1, 2))) + 1e-06)
    step_change = -(step_rate * param_scale)[:, None, None] * update / clip_factor
    new_params = params + step_change
    return (new_params, step_change, permute(row_new, new_map), permute(col_new, new_map))
```

```python
import math

import jax
import jax.numpy as jnp
from jax import lax
from jax.experimental import pallas as pl
from jax.experimental.pallas import tpu as pltpu
from jax.sharding import PartitionSpec as P

STEP = 4
eps_square = 1e-30
clip_limit = 1.0
highest = lax.Precision.HIGHEST
code_limit = 32767.0
finish_vmem = 48 * 2**20


def exchange(value, axis, bit):
    size = lax.axis_size(axis)
    return lax.ppermute(value, axis, [(i, i ^ bit) for i in range(size)])


def bits(size):
    out, bit = [], 1
    while bit < size:
        out.append(bit)
        bit *= 2
    return out


def all_sum(value, steps):
    for axis, bit in steps:
        value = value + exchange(value, axis, bit)
    return value


def halves_sum(value, steps, cross):
    for axis, bit in steps:
        half = value.shape[1] // 2
        upper = (lax.axis_index(axis) // bit) % 2
        kept = lax.dynamic_slice_in_dim(value, upper * half, half, 1)
        given = lax.dynamic_slice_in_dim(value, (1 - upper) * half, half, 1)
        value = kept + exchange(given, axis, bit)
    value = all_sum(value, cross)
    for axis, bit in reversed(steps):
        upper = (lax.axis_index(axis) // bit) % 2 == 1
        other = exchange(value, axis, bit)
        value = jnp.concatenate(
            [jnp.where(upper, other, value), jnp.where(upper, value, other)], axis=1
        )
    return value


def select_block(whole, wanted, blocks):
    matrices = whole.shape[0]
    onehot = (wanted[:, None] == jnp.arange(blocks, dtype=jnp.int32)[None, :]).astype(jnp.float32)
    pieces = whole.reshape(matrices, blocks, whole.shape[1] // blocks)
    return jnp.einsum("mb,mbw->mw", onehot, pieces, precision=highest)


def finish_body(own, *refs):
    if own:
        g_ref, p_ref, a_ref, b_ref = refs[:4]
    else:
        g_ref, p_ref, s_ref, a_ref, b_ref = refs[:5]
    new_ref, change_ref = refs[-2:]
    width = g_ref.shape[2]
    for j in range(width // 128):
        cols = pl.ds(j * 128, 128)
        change = g_ref[0, :, cols].astype(jnp.float32) * (a_ref[0] * b_ref[0, :, cols])
        if own:
            weights = p_ref[0, :, cols]
        else:
            weights = p_ref[0, :, cols].astype(jnp.int32).astype(jnp.float32) * s_ref[0, :, cols]
        change_ref[0, :, cols] = change
        new_ref[0, :, cols] = weights + change


def row_tile(span, rows):
    return min(span, rows // 2) if span % (rows // 2) == 0 or span < rows // 2 else rows // 4


def finish(outs, grad, grad_at, weights, weights_at, scale, k, first, count, begin, span, a, b, shape):
    own = scale is None
    matrices, rows, cols, whole_rows = shape
    tile = row_tile(span, rows)
    row_at, row_blocks = begin // tile, rows // tile
    grad_at, grad_row = grad_at
    weights_at, weights_row = weights_at

    def source(at, row):
        if own:
            return lambda m, t: (first + m, row + t, lax.axis_index("col"))
        return lambda m, t: (at + m, row + t, 0)

    def target(m, t):
        return (first + m, (lax.axis_index("col") ^ k) * row_blocks + row_at + t, 0)

    block = pl.BlockSpec((1, tile, cols), source(grad_at, grad_row // tile))
    block_w = pl.BlockSpec((1, tile, cols), source(weights_at, weights_row // tile))
    line = pl.BlockSpec((1, 1, cols), lambda m, t: (first + m, 0, 0))
    factor = pl.BlockSpec((1, tile, 128), target)
    result = pl.BlockSpec((1, tile, cols), target)
    args = [grad, weights] + ([] if own else [scale]) + [a, b]
    specs = [block, block_w] + ([] if own else [line]) + [factor, line]
    aliases = {}
    if outs is not None:
        aliases = {len(args): 0, len(args) + 1: 1}
        args += list(outs)
        specs += [pl.BlockSpec(memory_space=pl.ANY)] * 2
    out = jax.ShapeDtypeStruct((matrices, whole_rows, cols), jnp.float32)
    size = count * span * cols
    return pl.pallas_call(
        lambda *refs: finish_body(own, *refs),
        grid=(count, span // tile),
        in_specs=specs,
        out_specs=[result, result],
        out_shape=(out, out),
        input_output_aliases=aliases,
        compiler_params=pltpu.CompilerParams(vmem_limit_bytes=finish_vmem),
        cost_estimate=pl.CostEstimate(flops=4 * size, bytes_accessed=12 * size, transcendentals=0),
    )(*args)


def cut_body(*refs):
    half = len(refs) // 2
    for source, out in zip(refs[:half], refs[half:]):
        out[...] = source[...]


def cut(array, ks, first, count, begin, span, cols):
    tile = row_tile(span, array.shape[1])
    row_at = begin // tile

    def source(k):
        return pl.BlockSpec((1, tile, cols), lambda m, t: (first + m, row_at + t, lax.axis_index("col") ^ k))

    out = jax.ShapeDtypeStruct((count, span, cols), array.dtype)
    size = count * span * cols * len(ks)
    return pl.pallas_call(
        cut_body,
        grid=(count, span // tile),
        in_specs=[source(k) for k in ks],
        out_specs=[pl.BlockSpec((1, tile, cols), lambda m, t: (m, t, 0)) for _ in ks],
        out_shape=[out for _ in ks],
        cost_estimate=pl.CostEstimate(flops=size, bytes_accessed=4 * size, transcendentals=0),
    )(*[array for _ in ks])


def grad_chunks(matrices, rows):
    return [(0, 1, 0, rows), (1, 1, 0, rows), (2, matrices - 2, 0, rows)]


def weight_chunks(matrices, rows):
    last = matrices - 1
    high = rows - max(16, rows // 4)
    return [(0, 1, 0, rows), (1, last - 1, 0, rows), (last, 1, 0, high), (last, 1, high, rows - high)]


def step(params, grads, row_state_old, col_state_old, old_map, new_map):
    decay_rate = 1.0 - float(STEP) ** (-0.8)
    step_rate = min(0.01, 1.0 / math.sqrt(STEP))
    row_count = lax.axis_size("row")
    col_count = lax.axis_size("col")
    blocks = row_count * col_count
    matrices, rows, width = grads.shape
    depth = rows * blocks
    cols = width // col_count
    me_col = lax.axis_index("col")
    me_row = lax.axis_index("row")
    flat_index = lax.axis_index(("row", "col"))
    far = range(2, col_count)


    g_far = []
    for i, (first, count, begin, span) in enumerate(grad_chunks(matrices, rows)):
        groups = [[k] for k in far] if i == 0 else [list(far)]
        cuts = [x for ks in groups for x in cut(grads, ks, first, count, begin, span, cols)]
        g_far.append({k: exchange(x, "col", k) for k, x in zip(far, cuts)})
    near_cut = cut(grads, [1], 0, matrices, 0, rows, cols)[0]
    g_core = exchange(near_cut, "col", 1)

    gradient = grads.astype(jnp.float32)
    squares = gradient * gradient
    row_total, col_total = jnp.sum(squares, axis=2), jnp.sum(squares, axis=1)
    row_part = (row_total + width * eps_square) * ((1.0 - decay_rate) / width)
    col_part = (col_total + rows * eps_square) * ((1.0 - decay_rate) / depth)
    ids = jnp.arange(blocks, dtype=jnp.int32)
    held = lax.dynamic_slice_in_dim(old_map, flat_index, 1, 1)
    at_old = (held == ids[None, :]).astype(jnp.float32)
    at_own = (ids == flat_index).astype(jnp.float32)
    row_terms = (
        at_own[None, :, None] * row_part[:, None, :]
        + (decay_rate * at_old)[:, :, None] * row_state_old[:, None, :]
    ).reshape(matrices, depth)
    old_cols = ((decay_rate * at_old)[:, :, None] * col_state_old[:, None, :]).reshape(matrices, width)
    terms = jnp.concatenate([row_terms, col_part + old_cols], axis=1)
    far_bits = [("col", bit) for bit in reversed(bits(col_count)) if bit > 1]
    near_bits = [("row", bit) for bit in bits(row_count)] + [("col", 1)]
    new = halves_sum(terms, [("col", 1)] + near_bits[:-1], far_bits)
    row_new, col_new = new[:, :depth], new[:, depth:]
    row_mean = jnp.mean(row_new, axis=1)

    top = jnp.max(jnp.abs(params), axis=1)
    param_part = jnp.sum(params * params, axis=(1, 2))
    rounded = jnp.maximum(top * ((1.0 + 2.0**-7) / code_limit), 2.0**-125)
    rounded = lax.reduce_precision(rounded, exponent_bits=8, mantissa_bits=7)
    scale = rounded.astype(jnp.bfloat16)
    inverse = 1.0 / rounded

    def coded(first, count, k, begin=0, span=rows):
        left = (me_col ^ k) * cols
        inv = lax.dynamic_slice(inverse, (first, left), (count, cols))
        piece = lax.dynamic_slice(params, (first, begin, left), (count, span, cols))
        return jnp.round(piece * inv[:, None, :]).astype(jnp.int16)

    def scale_from(k):
        mine = lax.dynamic_slice_in_dim(scale, (me_col ^ k) * cols, cols, 1)
        return exchange(mine, "col", k)

    scales = {k: scale_from(k) for k in range(1, col_count)}
    p_core = exchange(coded(0, matrices, 1), "col", 1)
    p_far = []
    for first, count, begin, span in weight_chunks(matrices, rows):
        p_far.append({k: exchange(coded(first, count, k, begin, span), "col", k) for k in far})

    mine = lax.dynamic_slice_in_dim(row_new, flat_index * rows, rows, 1)
    update_part = jnp.sum(squares * (1.0 / mine)[:, :, None] * (1.0 / col_new)[:, None, :], axis=(1, 2))
    update_part = jnp.sum(update_part * row_mean)
    both = jnp.concatenate([param_part, update_part[None]])
    both = jnp.pad(both, (0, 128 - matrices - 1))[None, :]
    both = all_sum(both, near_bits + far_bits)[0]
    scales, both = lax.optimization_barrier((scales, both))
    scales = {k: x.astype(jnp.float32)[:, None, :] for k, x in scales.items()}
    clip_factor = jnp.maximum(1.0, jnp.sqrt(both[matrices] / (matrices * depth * width)) / clip_limit)
    param_scale = jnp.sqrt(both[:matrices] / (depth * width) + 1e-06)
    factor = -(step_rate * param_scale) / clip_factor * jnp.sqrt(row_mean)

    here_rows = rows * col_count
    a = factor[:, None] * lax.rsqrt(lax.dynamic_slice_in_dim(row_new, me_row * here_rows, here_rows, 1))
    a = jnp.broadcast_to(a[:, :, None], (matrices, here_rows, 128))
    b = lax.rsqrt(lax.dynamic_slice_in_dim(col_new, me_col * cols, cols, 1))[:, None, :]

    common = (a, b, (matrices, rows, cols, here_rows))
    outs = finish(None, grads, (0, 0), params, (0, 0), None, 0, 0, matrices, 0, rows, *common)
    outs = finish(outs, g_core, (0, 0), p_core, (0, 0), scales[1], 1, 0, matrices, 0, rows, *common)
    for i, (lead, number, begin, span) in enumerate(weight_chunks(matrices, rows)):
        for m, k in [(m, k) for k in far for m in range(lead, lead + number)]:
            for j, (first, count, top_row, height) in enumerate(grad_chunks(matrices, rows)):
                low, high = max(begin, top_row), min(begin + span, top_row + height)
                if first <= m < first + count and low < high:
                    grad_at, weights_at = (m - first, low - top_row), (m - lead, low - begin)
                    outs = finish(
                        outs, g_far[j][k], grad_at, p_far[i][k], weights_at,
                        scales[k], k, m, 1, low, high - low, *common,
                    )

    wanted = lax.dynamic_slice_in_dim(new_map, flat_index, 1, 1)[:, 0]
    row_state = select_block(row_new, wanted, blocks)
    col_state = select_block(col_new, wanted, blocks)
    return (outs[0], outs[1], row_state, col_state)


def solution(mesh):
    placed = (
        P(None, ("row", "col"), None),
        P(None, ("row", "col"), None),
        P(None, ("row", "col")),
        P(None, ("row", "col")),
        P(),
        P(),
    )
    return jax.shard_map(
        step,
        mesh=mesh,
        in_specs=placed,
        out_specs=(
            P(None, "row", "col"),
            P(None, "row", "col"),
            P(None, ("row", "col")),
            P(None, ("row", "col")),
        ),
        check_vma=False,
    )
```
